32 devices in a mesh: gy: 4 (over z), gz: 8 (over y, x, core).
Axes of the slice: x: 2, y: 2, z: 4, core: 2. Of those that a mesh axis runs over, the one named last changes fastest.
Arguments:
- data_weight: float32 [320, 160, 640], P('gy', 'gz'), may hold values from 0.25 to 4
- blob_taps: float32 [3, 7], replicated, may hold values from 0.2 to 1
Outputs:
- new_weight: float32 [320, 160, 640], P('gy', 'gz')
- changes: float32 [3], replicated
The draws below stay inside these ranges and needn't reach their ends.
All inputs are finite; a program needn't handle non-finite values.
Results may differ from the reference program's by a relative error of at most 0.00002.
Values sent between devices are 32-bit elements; how exact they have to be, the bound alone decides.
A program may use at most 64 MiB of HBM per device.

```python
import math
import jax
import jax.numpy as jnp
from jax import lax

XLEN = 640
RAD = 3
TAPS = 7
ITERS = 3
YLEN = 320
ZLEN = 160


def level_of(key, extent, shards, least, largest):
    gain = 1.0
    for axis_at, parts in shards:
        heights = jax.random.uniform(jax.random.fold_in(jax.random.fold_in(key, 6), axis_at), (parts,), jnp.float32, least / len(shards), largest / len(shards))
        gain = gain * jnp.repeat(jnp.exp(heights), extent[axis_at] // parts).reshape((-1,) + (1,) * (len(extent) - 1 - axis_at))
    return gain


def setup_inputs(seed: int = 0) -> dict:
    arg_keys = jax.random.split(jax.random.key(seed), 3)
    return {
        "data_weight": jnp.clip(jnp.exp(math.log(4.0) - 2.7725887 * jax.random.uniform(arg_keys[0], (YLEN, ZLEN, XLEN), jnp.float32) ** level_of(arg_keys[0], (YLEN, ZLEN, XLEN), ((0, 4), (1, 8)), -0.2, 0.2)), 0.25, 4.0),
        "blob_taps": jnp.clip(jax.random.uniform(arg_keys[1], (3, TAPS), jnp.float32, 0.2, 1.0), 0.2, 1.0),
    }


def smear_axis(field, kernel, axis_dim):
    length = field.shape[axis_dim]
    widths = [(0, 0), (0, 0), (0, 0)]
    widths[axis_dim] = (RAD, RAD)
    padded = jnp.pad(field, widths)
    result = jnp.zeros_like(field)
    for offset in range(2 * RAD + 1):
        result = result + kernel[offset] * lax.slice_in_dim(padded, offset, offset + length, axis=axis_dim)
    return result


def reference(data_weight, blob_taps):
    kernel = blob_taps / jnp.sum(blob_taps, axis=1, keepdims=True)
    weight = jnp.ones_like(data_weight)
    changes = []
    for iteration in range(ITERS):
        product = weight * data_weight
        blurred = smear_axis(product, kernel[2], 2)
        blurred = smear_axis(blurred, kernel[0], 0)
        blurred = smear_axis(blurred, kernel[1], 1)
        weight = weight / blurred
        changes.append(jnp.max(jnp.abs(blurred - 1.0)))
    return weight, jnp.stack(changes)
```

```python
import functools

import jax
import jax.numpy as jnp
from jax import lax
from jax.experimental import pallas as pl
from jax.experimental.pallas import tpu as pltpu
from jax.sharding import PartitionSpec as P

RAD = 3
ITERS = 3
TAPS = 2 * RAD + 1
LANES = 128
PAD = 8


def body(
    taps_ref, d_hbm, o_hbm, c_ref,
    D, W, Q, T, S, ZR, YSB, YRB, YSI, YRI, M, CS, CR1, CR2,
    in_sem, out_sem, zs, zr, ysb, yrb, ysi, yri, cs1, cr1, cs2, cr2,
):
    ny, nz, xlen = d_hbm.shape
    nb = xlen // LANES
    n_in = nz - 2 * RAD
    gy_n, gz_n = lax.axis_size("gy"), lax.axis_size("gz")
    gy, gz = lax.axis_index("gy"), lax.axis_index("gz")
    y_has = (gy > 0, gy < gy_n - 1)
    z_has = (gz > 0, gz < gz_n - 1)
    step = 16 if ny % 16 == 0 else 8

    barrier = pltpu.get_barrier_semaphore()
    for off in range(1, gy_n):
        pl.semaphore_signal(barrier, inc=1, device_id={"gy": lax.rem(gy + off, gy_n)})
    for off in range(1, gz_n):
        pl.semaphore_signal(barrier, inc=1, device_id={"gz": lax.rem(gz + off, gz_n)})

    edge_planes = list(range(RAD)) + list(range(nz - RAD, nz))
    inner_planes = list(range(RAD, nz - RAD))

    def in_copy(z, b):
        return pltpu.make_async_copy(
            d_hbm.at[:, z, pl.ds(b * LANES, LANES)], D.at[z, b + 1], in_sem.at[z, b]
        )

    def out_copy(z, b):
        return pltpu.make_async_copy(
            W.at[z, b], o_hbm.at[:, z, pl.ds(b * LANES, LANES)], out_sem.at[z, b]
        )

    for b in range(nb):
        for z in edge_planes:
            in_copy(z, b).start()
    for b in range(nb):
        for z in inner_planes:
            in_copy(z, b).start()

    blank = jnp.zeros((ny, LANES), jnp.float32)

    @pl.loop(0, nz)
    def _(z):
        for ref in (D, Q):
            ref[z, 0] = blank
            ref[z, nb + 1] = blank

    for side in range(2):
        @pl.when(jnp.logical_not(z_has[side]))
        def _():
            @pl.loop(0, ITERS * RAD)
            def _(i):
                for b in range(nb):
                    ZR[i // RAD, side, lax.rem(i, RAD), b] = blank

        @pl.when(jnp.logical_not(y_has[side]))
        def _():
            for it in range(ITERS):
                YRB[it, side] = jnp.zeros(YRB.shape[2:], jnp.float32)
                YRI[it, side] = jnp.zeros(YRI.shape[2:], jnp.float32)

    M[...] = jnp.zeros(M.shape, jnp.float32)
    CS[...] = jnp.zeros(CS.shape, jnp.float32)

    def tap_row(row):
        total = taps_ref[row, 0]
        for k in range(1, TAPS):
            total = total + taps_ref[row, k]
        bottom = jnp.full((8, LANES), total, jnp.float32)
        return [jnp.full((8, LANES), taps_ref[row, k], jnp.float32) / bottom for k in range(TAPS)]

    taps_y, taps_z, taps_x = tap_row(0), tap_row(1), tap_row(2)

    def wide(tap, rows):
        return tap if rows == 8 else jnp.concatenate([tap] * (rows // 8), axis=0)

    lane = lax.broadcasted_iota(jnp.int32, (step, LANES), 1)

    def plane_of(i):
        return i + (i // RAD) * n_in

    def smear_x(src, it, b, edge):
        kx = [wide(t, step) for t in taps_x]

        @pl.loop(0, 2 * RAD if edge else n_in)
        def _(i):
            z = plane_of(i) if edge else i + RAD
            for r in range(0, ny, step):
                rows = pl.ds(r, step)
                mid = src[z, b + 1, rows, :]
                left = src[z, b, rows, :]
                right = src[z, b + 2, rows, :]
                total = kx[RAD] * mid
                for s in range(1, RAD + 1):
                    up = pltpu.roll(jnp.where(lane < s, right, mid), LANES - s, 1)
                    down = pltpu.roll(jnp.where(lane >= LANES - s, left, mid), s, 1)
                    total = total + kx[RAD + s] * up + kx[RAD - s] * down
                T[z, b, pl.ds(PAD + r, step), :] = total
                send = YSB if edge else YSI
                if r == 0:
                    send[it, 0, b, i] = total[:RAD]
                if r + step == ny:
                    send[it, 1, b, i] = total[step - RAD:]

    def y_copy(it, to, b, edge):
        if edge:
            src, dst = YSB.at[it, to, b], YRB.at[it, 1 - to, b]
            ss, rs = ysb.at[it, to, b], yrb.at[it, 1 - to, b]
        else:
            src, dst = YSI.at[it, to], YRI.at[it, 1 - to]
            ss, rs = ysi.at[it, to], yri.at[it, 1 - to]
        peer = jnp.clip(gy + (1 if to else -1), 0, gy_n - 1)
        return pltpu.make_async_remote_copy(
            src_ref=src, dst_ref=dst, send_sem=ss, recv_sem=rs, device_id={"gy": peer}
        )

    def z_copy(it, to, b):
        first = nz - RAD if to else 0
        peer = jnp.clip(gz + (1 if to else -1), 0, gz_n - 1)
        return pltpu.make_async_remote_copy(
            src_ref=S.at[it, pl.ds(first, RAD), b],
            dst_ref=ZR.at[it, 1 - to, :, b],
            send_sem=zs.at[it, to, b],
            recv_sem=zr.at[it, 1 - to, b],
            device_id={"gz": peer},
        )

    def start(copy, has, *args):
        for to in range(2):
            @pl.when(has[to])
            def _():
                copy(args[0], to, *args[1:]).start()

    def arrived(copy, has, *args):
        for to in range(2):
            @pl.when(has[1 - to])
            def _():
                copy(args[0], to, *args[1:]).wait_recv()

    def sent(copy, has, *args):
        for to in range(2):
            @pl.when(has[to])
            def _():
                copy(args[0], to, *args[1:]).wait_send()

    def smear_y(it, b, edge):
        got = YRB if edge else YRI
        ky = [wide(t, step) for t in taps_y]

        @pl.loop(0, 2 * RAD if edge else n_in)
        def _(i):
            z = plane_of(i) if edge else i + RAD
            T[z, b, pl.ds(PAD - RAD, RAD), :] = got[it, 0, b, i]
            T[z, b, pl.ds(PAD + ny, RAD), :] = got[it, 1, b, i]
            for r in range(0, ny, step):
                total = ky[0] * T[z, b, pl.ds(PAD - RAD + r, step), :]
                for k in range(1, TAPS):
                    total = total + ky[k] * T[z, b, pl.ds(PAD - RAD + r + k, step), :]
                S[it, z, b, pl.ds(r, step), :] = total

    def smear_z(it, b, planes):
        kz = taps_z

        @pl.loop(0, ny // 8)
        def _(j):
            rows = pl.ds(pl.multiple_of(j * 8, 8), 8)
            needed = sorted({z + k - RAD for z in planes for k in range(TAPS)})
            got = {}
            for z in needed:
                if z < 0:
                    got[z] = ZR[it, 0, z + RAD, b, rows, :]
                elif z >= nz:
                    got[z] = ZR[it, 1, z - nz, b, rows, :]
                else:
                    got[z] = S[it, z, b, rows, :]
            most = M[it]
            for z in planes:
                blurred = kz[0] * got[z - RAD]
                for k in range(1, TAPS):
                    blurred = blurred + kz[k] * got[z + k - RAD]
                most = jnp.maximum(most, jnp.abs(blurred - 1.0))
                weight = (1.0 if it == 0 else W[z, b, rows, :]) / blurred
                W[z, b, rows, :] = weight
                if it < ITERS - 1:
                    Q[z, b + 1, rows, :] = weight * D[z, b + 1, rows, :]
            M[it] = most

    pl.semaphore_wait(barrier, gy_n - 1 + gz_n - 1)

    def ready(b, planes):
        if b < nb:
            for z in planes:
                in_copy(z, b).wait()

    ready(0, edge_planes)
    for b in range(nb):
        ready(b + 1, edge_planes)
        smear_x(D, 0, b, True)
        start(y_copy, y_has, 0, b, True)
        if b >= 1:
            arrived(y_copy, y_has, 0, b - 1, True)
            smear_y(0, b - 1, True)
            start(z_copy, z_has, 0, b - 1)
    for b in range(nb):
        ready(b, inner_planes)
    for b in range(nb):
        smear_x(D, 0, b, False)
        if b == 0:
            arrived(y_copy, y_has, 0, nb - 1, True)
            smear_y(0, nb - 1, True)
            start(z_copy, z_has, 0, nb - 1)
    start(y_copy, y_has, 0, 0, False)

    for it in range(ITERS):
        last = it == ITERS - 1
        arrived(y_copy, y_has, it, 0, False)
        for b in range(nb):
            smear_y(it, b, False)
        for b in range(nb):
            smear_z(it, b, inner_planes)
            if last:
                for z in inner_planes:
                    out_copy(z, b).start()
        if not last:
            for b in range(nb):
                smear_x(Q, it + 1, b, False)
            start(y_copy, y_has, it + 1, 0, False)
        for b in range(nb):
            arrived(z_copy, z_has, it, b)
            smear_z(it, b, edge_planes)
            if last:
                for z in edge_planes:
                    out_copy(z, b).start()
                continue
            if b >= 1:
                smear_x(Q, it + 1, b - 1, True)
                start(y_copy, y_has, it + 1, b - 1, True)
            if b >= 2:
                arrived(y_copy, y_has, it + 1, b - 2, True)
                smear_y(it + 1, b - 2, True)
                start(z_copy, z_has, it + 1, b - 2)
        if not last:
            smear_x(Q, it + 1, nb - 1, True)
            start(y_copy, y_has, it + 1, nb - 1, True)
            for b in (nb - 2, nb - 1):
                arrived(y_copy, y_has, it + 1, b, True)
                smear_y(it + 1, b, True)
                start(z_copy, z_has, it + 1, b)

    def c_copy(axis, me, count, off):
        src, dst, ss, rs = (CS.at[0], CR1, cs1, cr1) if axis == "gy" else (CS.at[1], CR2, cs2, cr2)
        return pltpu.make_async_remote_copy(
            src_ref=src, dst_ref=dst.at[off], send_sem=ss.at[off], recv_sem=rs.at[off],
            device_id={axis: lax.rem(me + off, count)},
        )

    for it in range(ITERS):
        CS[0, it:it + 1] = jnp.max(M[it], axis=0, keepdims=True)
    for off in range(1, gy_n):
        c_copy("gy", gy, gy_n, off).start()
    most = CS[0]
    for off in range(1, gy_n):
        c_copy("gy", gy, gy_n, off).wait_recv()
        most = jnp.maximum(most, CR1[off])
    CS[1] = most
    for off in range(1, gz_n):
        c_copy("gz", gz, gz_n, off).start()
    for off in range(1, gz_n):
        c_copy("gz", gz, gz_n, off).wait_recv()
        most = jnp.maximum(most, CR2[off])
    for it in range(ITERS):
        c_ref[it] = jnp.max(most[it:it + 1])

    for it in range(ITERS):
        for b in range(nb):
            sent(y_copy, y_has, it, b, True)
            sent(z_copy, z_has, it, b)
        sent(y_copy, y_has, it, 0, False)
    for off in range(1, gy_n):
        c_copy("gy", gy, gy_n, off).wait_send()
    for off in range(1, gz_n):
        c_copy("gz", gz, gz_n, off).wait_send()
    for z in inner_planes + edge_planes:
        for b in range(nb):
            out_copy(z, b).wait()


def shards(data_weight, blob_taps):
    ny, nz, xlen = data_weight.shape
    nb = xlen // LANES
    n_in = nz - 2 * RAD
    gy_n, gz_n = lax.axis_size("gy"), lax.axis_size("gz")
    f32, vmem, dma = jnp.float32, pltpu.VMEM, pltpu.SemaphoreType.DMA
    return pl.pallas_call(
        body,
        out_shape=(
            jax.ShapeDtypeStruct(data_weight.shape, f32),
            jax.ShapeDtypeStruct((ITERS,), f32),
        ),
        in_specs=[
            pl.BlockSpec(memory_space=pltpu.SMEM),
            pl.BlockSpec(memory_space=pl.ANY),
        ],
        out_specs=(
            pl.BlockSpec(memory_space=pl.ANY),
            pl.BlockSpec(memory_space=pltpu.SMEM),
        ),
        scratch_shapes=[
            vmem((nz, nb + 2, ny, LANES), f32),
            vmem((nz, nb, ny, LANES), f32),
            vmem((nz, nb + 2, ny, LANES), f32),
            vmem((nz, nb, ny + 2 * PAD, LANES), f32),
            vmem((ITERS, nz, nb, ny, LANES), f32),
            vmem((ITERS, 2, RAD, nb, ny, LANES), f32),
            vmem((ITERS, 2, nb, 2 * RAD, RAD, LANES), f32),
            vmem((ITERS, 2, nb, 2 * RAD, RAD, LANES), f32),
            vmem((ITERS, 2, nb, n_in, RAD, LANES), f32),
            vmem((ITERS, 2, nb, n_in, RAD, LANES), f32),
            vmem((ITERS, 8, LANES), f32),
            vmem((2, 8, LANES), f32),
            vmem((gy_n, 8, LANES), f32),
            vmem((gz_n, 8, LANES), f32),
            dma((nz, nb)),
            dma((nz, nb)),
            dma((ITERS, 2, nb)),
            dma((ITERS, 2, nb)),
            dma((ITERS, 2, nb)),
            dma((ITERS, 2, nb)),
            dma((ITERS, 2)),
            dma((ITERS, 2)),
            dma((gy_n,)),
            dma((gy_n,)),
            dma((gz_n,)),
            dma((gz_n,)),
        ],
        compiler_params=pltpu.CompilerParams(
            collective_id=0, has_side_effects=True, vmem_limit_bytes=62 * 1024 * 1024
        ),
        name="gridding",
    )(blob_taps, data_weight)


def solution(mesh):
    return jax.shard_map(
        shards,
        mesh=mesh,
        in_specs=(P("gy", "gz", None), P()),
        out_specs=(P("gy", "gz", None), P()),
        check_vma=False,
    )
```

```python
import functools

import jax
import jax.numpy as jnp
from jax import lax
from jax.experimental import pallas as pl
from jax.experimental.pallas import tpu as pltpu
from jax.sharding import PartitionSpec as P

RAD = 3
ITERS = 3
TAPS = 2 * RAD + 1
LANES = 128
PAD = 8


def body(
    taps_ref, d_hbm, o_hbm, c_ref,
    KX, D, W, Q, T, S, ZR, YSB, YRB, YSI, YRI, M, CS, CR1, CR2,
    in_sem, out_sem, zs, zr, ysb, yrb, ysi, yri, cs1, cr1, cs2, cr2,
):
    nz, ny, xlen = d_hbm.shape
    nb = xlen // LANES
    n_in = nz - 2 * RAD
    gy_n, gz_n = lax.axis_size("gy"), lax.axis_size("gz")
    gy, gz = lax.axis_index("gy"), lax.axis_index("gz")
    y_has = (gy > 0, gy < gy_n - 1)
    z_has = (gz > 0, gz < gz_n - 1)
    step = 16 if ny % 16 == 0 else 8

    barrier = pltpu.get_barrier_semaphore()
    for off in range(1, gy_n):
        pl.semaphore_signal(barrier, inc=1, device_id={"gy": lax.rem(gy + off, gy_n)})
    for off in range(1, gz_n):
        pl.semaphore_signal(barrier, inc=1, device_id={"gz": lax.rem(gz + off, gz_n)})

    edge_planes = list(range(RAD)) + list(range(nz - RAD, nz))
    inner_planes = list(range(RAD, nz - RAD))

    def in_copy(z, b):
        return pltpu.make_async_copy(
            d_hbm.at[z, :, pl.ds(b * LANES, LANES)], D.at[z, b + 1], in_sem.at[z, b]
        )

    def out_copy(z, b):
        return pltpu.make_async_copy(
            W.at[z, b], o_hbm.at[z, :, pl.ds(b * LANES, LANES)], out_sem.at[z, b]
        )

    for b in range(nb):
        for z in edge_planes:
            in_copy(z, b).start()
    for b in range(nb):
        for z in inner_planes:
            in_copy(z, b).start()

    blank = jnp.zeros((ny, LANES), jnp.float32)

    @pl.loop(0, nz)
    def _(z):
        for ref in (D, Q):
            ref[z, 0] = blank
            ref[z, nb + 1] = blank

    for side in range(2):
        @pl.when(jnp.logical_not(z_has[side]))
        def _():
            @pl.loop(0, ITERS * RAD)
            def _(i):
                for b in range(nb):
                    ZR[i // RAD, side, lax.rem(i, RAD), b] = blank

        @pl.when(jnp.logical_not(y_has[side]))
        def _():
            for it in range(ITERS):
                YRB[it, side] = jnp.zeros(YRB.shape[2:], jnp.float32)
                YRI[it, side] = jnp.zeros(YRI.shape[2:], jnp.float32)

    M[...] = jnp.zeros(M.shape, jnp.float32)
    CS[...] = jnp.zeros(CS.shape, jnp.float32)

    def tap_row(row):
        total = taps_ref[row, 0]
        for k in range(1, TAPS):
            total = total + taps_ref[row, k]
        bottom = jnp.full((8, LANES), total, jnp.float32)
        return [jnp.full((8, LANES), taps_ref[row, k], jnp.float32) / bottom for k in range(TAPS)]

    taps_y, taps_z, taps_x = tap_row(0), tap_row(1), tap_row(2)

    def wide(tap, rows):
        return tap if rows == 8 else jnp.concatenate([tap] * (rows // 8), axis=0)

    row = lax.broadcasted_iota(jnp.int32, (LANES, LANES), 0)
    gap = row - lax.broadcasted_iota(jnp.int32, (LANES, LANES), 1)
    for part in range(2):
        taps = jnp.zeros((LANES, LANES), jnp.float32)
        for k in range(TAPS):
            tap = wide(taps_x[k], LANES)
            if part == 0:
                taps = jnp.where(gap == k - RAD, tap, taps)
            elif k < RAD:
                taps = jnp.where(gap == k - RAD + LANES, tap, taps)
            elif k > RAD:
                taps = jnp.where(gap == k - RAD - LANES, tap, taps)
        large = taps.astype(jnp.bfloat16)
        small = (taps - large.astype(jnp.float32)).astype(jnp.bfloat16)
        both = jnp.concatenate([large, small], axis=1)
        KX[pl.ds(part * LANES, LANES), :] = both
        KX[pl.ds((2 + part) * LANES, LANES), :] = both

    near = lax.broadcasted_iota(jnp.int32, (ny, LANES), 1) < LANES // 2

    def plane_of(i):
        return i + (i // RAD) * n_in

    def smear_x(src, it, b, edge):
        send = YSB if edge else YSI
        group = RAD if edge else (7 if n_in % 7 == 0 else 1)

        @pl.loop(0, (2 * RAD if edge else n_in) // group)
        def _(step_at):
            first = step_at * (n_in + RAD) if edge else RAD + step_at * group
            rows = []
            for g in range(group):
                z = first + g
                fringe = jnp.where(near, src[z, b + 2], src[z, b])
                cells = jnp.concatenate([src[z, b + 1], fringe], axis=1)
                large = cells.astype(jnp.bfloat16)
                small = (cells - large.astype(jnp.float32)).astype(jnp.bfloat16)
                rows.append(jnp.concatenate([large, small], axis=1))
            made = jnp.dot(
                jnp.concatenate(rows, axis=0), KX[...], preferred_element_type=jnp.float32
            )
            total = made[:, :LANES] + made[:, LANES:]
            for g in range(group):
                plane = total[g * ny:(g + 1) * ny]
                T[first + g, b, pl.ds(PAD, ny), :] = plane
                send[it, 0, b, step_at * group + g] = plane[:RAD]
                send[it, 1, b, step_at * group + g] = plane[ny - RAD:]

    def y_copy(it, to, b, edge):
        if edge:
            src, dst = YSB.at[it, to, b], YRB.at[it, 1 - to, b]
            ss, rs = ysb.at[it, to, b], yrb.at[it, 1 - to, b]
        else:
            src, dst = YSI.at[it, to], YRI.at[it, 1 - to]
            ss, rs = ysi.at[it, to], yri.at[it, 1 - to]
        peer = jnp.clip(gy + (1 if to else -1), 0, gy_n - 1)
        return pltpu.make_async_remote_copy(
            src_ref=src, dst_ref=dst, send_sem=ss, recv_sem=rs, device_id={"gy": peer}
        )

    def z_copy(it, to, b):
        first = nz - RAD if to else 0
        peer = jnp.clip(gz + (1 if to else -1), 0, gz_n - 1)
        return pltpu.make_async_remote_copy(
            src_ref=S.at[it, pl.ds(first, RAD), b],
            dst_ref=ZR.at[it, 1 - to, :, b],
            send_sem=zs.at[it, to, b],
            recv_sem=zr.at[it, 1 - to, b],
            device_id={"gz": peer},
        )

    def start(copy, has, *args):
        for to in range(2):
            @pl.when(has[to])
            def _():
                copy(args[0], to, *args[1:]).start()

    def arrived(copy, has, *args):
        for to in range(2):
            @pl.when(has[1 - to])
            def _():
                copy(args[0], to, *args[1:]).wait_recv()

    def sent(copy, has, *args):
        for to in range(2):
            @pl.when(has[to])
            def _():
                copy(args[0], to, *args[1:]).wait_send()

    def smear_y(it, b, edge):
        got = YRB if edge else YRI
        ky = [wide(t, step) for t in taps_y]

        @pl.loop(0, 2 * RAD if edge else n_in)
        def _(i):
            z = plane_of(i) if edge else i + RAD
            T[z, b, pl.ds(PAD - RAD, RAD), :] = got[it, 0, b, i]
            T[z, b, pl.ds(PAD + ny, RAD), :] = got[it, 1, b, i]
            for r in range(0, ny, step):
                total = ky[0] * T[z, b, pl.ds(PAD - RAD + r, step), :]
                for k in range(1, TAPS):
                    total = total + ky[k] * T[z, b, pl.ds(PAD - RAD + r + k, step), :]
                S[it, z, b, pl.ds(r, step), :] = total

    def smear_z(it, b, planes):
        kz = taps_z

        @pl.loop(0, ny // 8)
        def _(j):
            rows = pl.ds(pl.multiple_of(j * 8, 8), 8)
            needed = sorted({z + k - RAD for z in planes for k in range(TAPS)})
            got = {}
            for z in needed:
                if z < 0:
                    got[z] = ZR[it, 0, z + RAD, b, rows, :]
                elif z >= nz:
                    got[z] = ZR[it, 1, z - nz, b, rows, :]
                else:
                    got[z] = S[it, z, b, rows, :]
            most = M[it]
            for z in planes:
                blurred = kz[0] * got[z - RAD]
                for k in range(1, TAPS):
                    blurred = blurred + kz[k] * got[z + k - RAD]
                most = jnp.maximum(most, jnp.abs(blurred - 1.0))
                weight = (1.0 if it == 0 else W[z, b, rows, :]) / blurred
                W[z, b, rows, :] = weight
                if it < ITERS - 1:
                    Q[z, b + 1, rows, :] = weight * D[z, b + 1, rows, :]
            M[it] = most

    pl.semaphore_wait(barrier, gy_n - 1 + gz_n - 1)

    def ready(b, planes):
        if b < nb:
            for z in planes:
                in_copy(z, b).wait()

    ready(0, edge_planes)
    for b in range(nb):
        ready(b + 1, edge_planes)
        smear_x(D, 0, b, True)
        start(y_copy, y_has, 0, b, True)
        if b >= 1:
            arrived(y_copy, y_has, 0, b - 1, True)
            smear_y(0, b - 1, True)
            start(z_copy, z_has, 0, b - 1)
    for b in range(nb):
        ready(b, inner_planes)
    for b in range(nb):
        smear_x(D, 0, b, False)
        if b == 0:
            arrived(y_copy, y_has, 0, nb - 1, True)
            smear_y(0, nb - 1, True)
            start(z_copy, z_has, 0, nb - 1)
    start(y_copy, y_has, 0, 0, False)

    for it in range(ITERS):
        last = it == ITERS - 1
        arrived(y_copy, y_has, it, 0, False)
        for b in range(nb):
            smear_y(it, b, False)
        for b in range(nb):
            smear_z(it, b, inner_planes)
            if last:
                for z in inner_planes:
                    out_copy(z, b).start()
        if not last:
            for b in range(nb):
                smear_x(Q, it + 1, b, False)
            start(y_copy, y_has, it + 1, 0, False)
        for b in range(nb):
            arrived(z_copy, z_has, it, b)
            smear_z(it, b, edge_planes)
            if last:
                for z in edge_planes:
                    out_copy(z, b).start()
                continue
            if b >= 1:
                smear_x(Q, it + 1, b - 1, True)
                start(y_copy, y_has, it + 1, b - 1, True)
            if b >= 2:
                arrived(y_copy, y_has, it + 1, b - 2, True)
                smear_y(it + 1, b - 2, True)
                start(z_copy, z_has, it + 1, b - 2)
        if not last:
            smear_x(Q, it + 1, nb - 1, True)
            start(y_copy, y_has, it + 1, nb - 1, True)
            for b in (nb - 2, nb - 1):
                arrived(y_copy, y_has, it + 1, b, True)
                smear_y(it + 1, b, True)
                start(z_copy, z_has, it + 1, b)

    def c_copy(axis, me, count, off):
        src, dst, ss, rs = (CS.at[0], CR1, cs1, cr1) if axis == "gy" else (CS.at[1], CR2, cs2, cr2)
        return pltpu.make_async_remote_copy(
            src_ref=src, dst_ref=dst.at[off], send_sem=ss.at[off], recv_sem=rs.at[off],
            device_id={axis: lax.rem(me + off, count)},
        )

    for it in range(ITERS):
        CS[0, it:it + 1] = jnp.max(M[it], axis=0, keepdims=True)
    for off in range(1, gy_n):
        c_copy("gy", gy, gy_n, off).start()
    most = CS[0]
    for off in range(1, gy_n):
        c_copy("gy", gy, gy_n, off).wait_recv()
        most = jnp.maximum(most, CR1[off])
    CS[1] = most
    for off in range(1, gz_n):
        c_copy("gz", gz, gz_n, off).start()
    for off in range(1, gz_n):
        c_copy("gz", gz, gz_n, off).wait_recv()
        most = jnp.maximum(most, CR2[off])
    for it in range(ITERS):
        c_ref[it] = jnp.max(most[it:it + 1])

    for it in range(ITERS):
        for b in range(nb):
            sent(y_copy, y_has, it, b, True)
            sent(z_copy, z_has, it, b)
        sent(y_copy, y_has, it, 0, False)
    for off in range(1, gy_n):
        c_copy("gy", gy, gy_n, off).wait_send()
    for off in range(1, gz_n):
        c_copy("gz", gz, gz_n, off).wait_send()
    for z in inner_planes + edge_planes:
        for b in range(nb):
            out_copy(z, b).wait()


def shards(data_weight, blob_taps):
    ny, nz, xlen = data_weight.shape
    nb = xlen // LANES
    n_in = nz - 2 * RAD
    gy_n, gz_n = lax.axis_size("gy"), lax.axis_size("gz")
    f32, vmem, dma = jnp.float32, pltpu.VMEM, pltpu.SemaphoreType.DMA
    weight, changes = pl.pallas_call(
        body,
        out_shape=(
            jax.ShapeDtypeStruct((nz, ny, xlen), f32),
            jax.ShapeDtypeStruct((ITERS,), f32),
        ),
        in_specs=[
            pl.BlockSpec(memory_space=pltpu.SMEM),
            pl.BlockSpec(memory_space=pl.ANY),
        ],
        out_specs=(
            pl.BlockSpec(memory_space=pl.ANY),
            pl.BlockSpec(memory_space=pltpu.SMEM),
        ),
        scratch_shapes=[
            vmem((4 * LANES, 2 * LANES), jnp.bfloat16),
            vmem((nz, nb + 2, ny, LANES), f32),
            vmem((nz, nb, ny, LANES), f32),
            vmem((nz, nb + 2, ny, LANES), f32),
            vmem((nz, nb, ny + 2 * PAD, LANES), f32),
            vmem((ITERS, nz, nb, ny, LANES), f32),
            vmem((ITERS, 2, RAD, nb, ny, LANES), f32),
            vmem((ITERS, 2, nb, 2 * RAD, RAD, LANES), f32),
            vmem((ITERS, 2, nb, 2 * RAD, RAD, LANES), f32),
            vmem((ITERS, 2, nb, n_in, RAD, LANES), f32),
            vmem((ITERS, 2, nb, n_in, RAD, LANES), f32),
            vmem((ITERS, 8, LANES), f32),
            vmem((2, 8, LANES), f32),
            vmem((gy_n, 8, LANES), f32),
            vmem((gz_n, 8, LANES), f32),
            dma((nz, nb)),
            dma((nz, nb)),
            dma((ITERS, 2, nb)),
            dma((ITERS, 2, nb)),
            dma((ITERS, 2, nb)),
            dma((ITERS, 2, nb)),
            dma((ITERS, 2)),
            dma((ITERS, 2)),
            dma((gy_n,)),
            dma((gy_n,)),
            dma((gz_n,)),
            dma((gz_n,)),
        ],
        compiler_params=pltpu.CompilerParams(
            collective_id=0, has_side_effects=True, vmem_limit_bytes=62 * 1024 * 1024
        ),
        name="gridding",
    )(blob_taps, jnp.transpose(data_weight, (1, 0, 2)))
    return jnp.transpose(weight, (1, 0, 2)), changes


def solution(mesh):
    return jax.shard_map(
        shards,
        mesh=mesh,
        in_specs=(P("gy", "gz", None), P()),
        out_specs=(P("gy", "gz", None), P()),
        check_vma=False,
    )
```
